32 devices in a mesh: row: 2 (over y), col: 4 (over z), depth: 4 (over x, core).
Axes of the slice: x: 2, y: 2, z: 4, core: 2. Of those that a mesh axis runs over, the one named last changes fastest.
Arguments:
- grad_out: bfloat16 [1024, 6144], P('depth', 'col'), may hold values from -6 to 6
- pre_act: bfloat16 [1024, 24576], P('depth', 'row'), may hold values from -8 to 8
- down_weight: bfloat16 [24576, 6144], P(('row', 'depth'), 'col'), may hold values from -0.0546875 to 0.0546875
Outputs:
- grad_pre: bfloat16 [1024, 24576], P('depth', 'row')
- grad_weight: bfloat16 [24576, 6144], P(('row', 'depth'), 'col')
The draws below stay inside these ranges and needn't reach their ends.
All inputs are finite; a program needn't handle non-finite values.
Results may differ from the reference program's by a relative error of at most 0.0066.
Values may be sent and summed in bfloat16 or wider, within the bound.
A program may use at most 128 MiB of HBM per device.

```python
import jax
import jax.numpy as jnp

D = 6144
FF = 24576
TOKENS = 1024


def with_spikes(values, rng, source, target, shards_of, factor):
    owner, partner = [(jnp.arange(values.shape[dim]) // (values.shape[dim] // shards_of)).reshape([-1 if axis == dim else 1 for axis in range(values.ndim)]) for dim in (source, target)]
    chosen = jax.random.permutation(rng, shards_of)[partner]
    strong = (owner == chosen) | (owner == (partner + shards_of // 2) % shards_of)
    return jnp.where(strong, factor * values, values)


def levels(stream_key, extent, cuts, low, largest):
    gain, own = 1.0, jax.random.fold_in(stream_key, 6)
    for position, parts in cuts:
        heights = jnp.exp(jax.random.uniform(jax.random.fold_in(own, position), (parts,), jnp.float32, low / len(cuts), largest / len(cuts)))
        gain = gain * jnp.repeat(heights, extent[position] // parts).reshape([-1 if axis == position else 1 for axis in range(len(extent))])
    return gain


def scatter_about(stream_key, dims, spread, bound, shards=(), held_as=jnp.bfloat16):
    entries = spread * jax.random.normal(stream_key, dims, jnp.float32)
    if shards:
        entries = entries * levels(stream_key, dims, shards, -0.22, 0.18)
    return jnp.clip(entries, -bound, bound).astype(held_as)


def gaussian_with(key, dims, spread, reach, pieces, heavy, held_as=jnp.bfloat16):
    drawn = spread * jax.random.normal(key, dims, jnp.float32)
    if pieces:
        drawn = drawn * levels(key, dims, pieces, -0.22, 0.18)
    return jnp.clip(with_spikes(drawn, jax.random.fold_in(key, 3), *heavy), -reach, reach).astype(held_as)


def setup_inputs(seed: int = 0) -> dict:
    arg_keys = jax.random.split(jax.random.key(seed), 4)
    grad_out = scatter_about(arg_keys[0], (TOKENS, D), 1.0, 6.0, ((0, 4), (1, 4)))
    pre_act = gaussian_with(arg_keys[1], (TOKENS, FF), 1.5, 8.0, ((0, 4), (1, 2)), (0, 1, 4, 2.0))
    down_weight = gaussian_with(arg_keys[2], (FF, D), FF ** -0.5, 0.0546875, ((0, 8), (1, 4)), (1, 0, 8, 2.0))
    return dict(grad_out=grad_out, pre_act=pre_act, down_weight=down_weight)


sqrt_two_pi = 0.7978845608028654
cubic_coeff = 0.044715

def gelu_value(preact):
    tangent = jnp.tanh(sqrt_two_pi * (preact + cubic_coeff * preact * preact * preact))
    return 0.5 * preact * (1.0 + tangent)

def gelu_slope(preact):
    tangent = jnp.tanh(sqrt_two_pi * (preact + cubic_coeff * preact * preact * preact))
    inner = sqrt_two_pi * (1.0 + 3.0 * cubic_coeff * preact * preact)
    return 0.5 * (1.0 + tangent) + 0.5 * preact * (1.0 - tangent * tangent) * inner

def reference(grad_out, pre_act, down_weight):
    widened = pre_act.astype(jnp.float32)
    activation = gelu_value(widened).astype(jnp.bfloat16)
    backward = jnp.dot(grad_out, down_weight.T, preferred_element_type=jnp.float32)
    grad_pre = (backward * gelu_slope(widened)).astype(jnp.bfloat16)
    grad_weight = jnp.dot(activation.T, grad_out, preferred_element_type=jnp.float32).astype(jnp.bfloat16)
    return (grad_pre, grad_weight)
```

```python
import jax
import jax.numpy as jnp
from jax import lax
from jax.sharding import PartitionSpec as P

sqrt_two_pi = 0.7978845608028654
cubic_coeff = 0.044715


def gelu_value(preact):
    tangent = jnp.tanh(sqrt_two_pi * (preact + cubic_coeff * preact * preact * preact))
    return 0.5 * preact * (1.0 + tangent)


def gelu_slope(preact):
    tangent = jnp.tanh(sqrt_two_pi * (preact + cubic_coeff * preact * preact * preact))
    inner = sqrt_two_pi * (1.0 + 3.0 * cubic_coeff * preact * preact)
    return 0.5 * (1.0 + tangent) + 0.5 * preact * (1.0 - tangent * tangent) * inner


def contract_last(left, right):
    return lax.dot_general(
        left, right, (((1,), (1,)), ((), ())), preferred_element_type=jnp.float32
    )


def contract_first(left, right):
    return lax.dot_general(
        left, right, (((0,), (0,)), ((), ())), preferred_element_type=jnp.float32
    )


def solution(mesh):
    cols = mesh.shape["col"]
    depths = mesh.shape["depth"]
    rounds = range(cols - 1)
    to_right = [(i, i + 1) for i in rounds]
    to_left = [(i + 1, i) for i in rounds]

    def on_device(grad_out, pre_act, down_weight):
        column = lax.axis_index("col")
        place = lax.axis_index("depth")
        block, width = grad_out.shape
        hidden = down_weight.shape[0]
        sub = block // cols

        def swap(value, step):
            return lax.ppermute(value, "depth", [(i, i ^ step) for i in range(depths)])

        def add(left, right):
            return left.astype(jnp.float32) + right.astype(jnp.float32)

        def pick(parts, which):
            return lax.dynamic_index_in_dim(
                parts, jnp.clip(which, 0, cols - 1), 0, keepdims=False
            )

        def scatter_round(parts, got, r):
            right = pick(parts, cols - 1 - r + column)
            left = pick(parts, r + column + 1 - cols)
            if got is not None:
                right = add(right, got[0]).astype(jnp.bfloat16)
                left = add(left, got[1]).astype(jnp.bfloat16)
            return (
                lax.ppermute(right, "col", [p for p in to_right if p[0] <= r]),
                lax.ppermute(left, "col", [p for p in to_left if cols - 1 - p[0] <= r]),
            )

        def gather_round(got, r):
            return (
                lax.ppermute(got[0], "col", [p for p in to_right if p[0] >= r]),
                lax.ppermute(got[1], "col", [p for p in to_left if cols - 1 - p[0] >= r]),
            )

        grads = [grad_out]
        for step in range(1, depths):
            if step & 1 and step > 1:
                grads.append(swap(grads[step ^ 1], 1))
            else:
                grads.append(swap(grad_out, step))
        pres = []
        for step in range(depths):
            part = lax.dynamic_slice_in_dim(pre_act, (place ^ step) * hidden, hidden, 1)
            pres.append(swap(part, step) if step else part)

        pairs = range(0, depths, 2)
        parts, ordered = [], []
        for base in pairs:
            two = jnp.stack([g.reshape(cols, sub, width) for g in grads[base : base + 2]], 1)
            two = two.reshape(2 * block, width)
            ordered.append(two)
            parts.append(
                contract_last(two, down_weight)
                .astype(jnp.bfloat16)
                .reshape(cols, 2 * sub, hidden)
            )
        got = [None for _ in pairs]
        for r in rounds:
            for pair in range(len(parts)):
                got[pair] = scatter_round(parts[pair], got[pair], r)

        pieces = []
        for pair, base in enumerate(pairs):
            total = add(pick(parts[pair], column), got[pair][0]) + got[pair][1].astype(jnp.float32)
            ends = []
            for k in range(2):
                seen = lax.dynamic_slice_in_dim(pres[base + k], column * sub, sub, 0)
                end = total[k * sub : (k + 1) * sub] * gelu_slope(seen.astype(jnp.float32))
                end = end.astype(jnp.bfloat16)
                ends.append(swap(end, base + k) if base + k else end)
            odd = ((place ^ base) & 1) == 1
            pieces.append(
                jnp.concatenate(
                    [jnp.where(odd, ends[1], ends[0]), jnp.where(odd, ends[0], ends[1])], 1
                )
            )

        grad_pre = jnp.zeros(pre_act.shape, jnp.bfloat16)
        sent = [(piece, piece) for piece in pieces]
        seen = [[] for _ in pairs]
        for r in rounds:
            for pair in range(len(pieces)):
                sent[pair] = gather_round(sent[pair], r)
                seen[pair].append(sent[pair])
        for pair, base in enumerate(pairs):
            offset = ((place ^ base) // 2) * 2 * hidden
            grad_pre = lax.dynamic_update_slice(
                grad_pre, pieces[pair], (column * sub, offset)
            )
            for r in rounds:
                rows = jnp.where(column > r, seen[pair][r][0], seen[pair][cols - 2 - r][1])
                source = lax.rem(column + cols - 1 - r, cols)
                grad_pre = lax.dynamic_update_slice(grad_pre, rows, (source * sub, offset))

        acts = []
        for base in pairs:
            two = jnp.stack([p.reshape(cols, sub, hidden) for p in pres[base : base + 2]], 1)
            two = two.reshape(2 * block, hidden)
            acts.append(gelu_value(two.astype(jnp.float32)).astype(jnp.bfloat16))
        grad_weight = contract_first(
            jnp.concatenate(acts), jnp.concatenate(ordered)
        ).astype(jnp.bfloat16)
        return (grad_pre, grad_weight)

    placed = (P("depth", "col"), P("depth", "row"), P(("row", "depth"), "col"))
    return jax.shard_map(
        on_device,
        mesh=mesh,
        in_specs=placed,
        out_specs=(P("depth", "row"), P(("row", "depth"), "col")),
        check_vma=False,
    )
```
